32 devices in a mesh: rep: 1 (over z), data: 32 (over y, x, core).
Axes of the slice: x: 4, y: 4, z: 1, core: 2. Of those that a mesh axis runs over, the one named last changes fastest.
The devices are a block of a 4x4x8 slice.
Arguments:
- x: bfloat16 [8192, 4096], P(('rep', 'data'))
- adapter_id: int32 [8192], P(('rep', 'data'))
- dout: bfloat16 [8192, 4096], P(('rep', 'data'))
- w_gate: bfloat16 [4096, 14336], replicated
- w_up: bfloat16 [4096, 14336], replicated
- w_down: bfloat16 [14336, 4096], replicated
- a_gate: bfloat16 [64, 4096, 32], P('data')
- b_gate: bfloat16 [64, 32, 14336], P('data')
- a_up: bfloat16 [64, 4096, 32], P('data')
- b_up: bfloat16 [64, 32, 14336], P('data')
- a_down: bfloat16 [64, 14336, 32], P('data')
- b_down: bfloat16 [64, 32, 4096], P('data')
Outputs:
- output 1: bfloat16 [8192, 4096], P(('rep', 'data'))
- output 2: bfloat16 [8192, 4096], P(('rep', 'data'))
- output 3: float32 [64, 4096, 32], P(('rep', 'data'))
- output 4: float32 [64, 32, 14336], P(('rep', 'data'))
- output 5: float32 [64, 4096, 32], P(('rep', 'data'))
- output 6: float32 [64, 32, 14336], P(('rep', 'data'))
- output 7: float32 [64, 14336, 32], P(('rep', 'data'))
- output 8: float32 [64, 32, 4096], P(('rep', 'data'))
All inputs are finite; a program needn't handle non-finite values.
Results may differ from the reference program's by a relative error of at most 0.00138.
Values are sent between devices in bfloat16 or wider.
A program may use at most 768 MiB of HBM per device.

```python
import jax
import jax.numpy as jnp
from jax import lax

TOKENS = 256
ADAPTERS = 2
MODEL_DIM = 4096
HIDDEN_DIM = 14336
LORA_RANK = 32
GROUP_SIZE = 32
CAPACITY = 24
LORA_ALPHA = 32
BLOCK_ROWS = 32

PART_TOKENS = TOKENS * GROUP_SIZE
NUM_ADAPTERS = ADAPTERS * GROUP_SIZE
LORA_SCALE = LORA_ALPHA / LORA_RANK


def draw_ids(rand_key):
    key_hot, key_off, key_shift, key_perm = jax.random.split(rand_key, 4)
    hot_owner = jax.random.randint(key_hot, (), 0, GROUP_SIZE)
    start_offset = jax.random.randint(key_off, (), 0, GROUP_SIZE - 1)
    owner_shift = jax.random.randint(key_shift, (GROUP_SIZE,), 0, ADAPTERS)
    spare_rows = TOKENS - CAPACITY
    source_dev = jnp.arange(GROUP_SIZE)[:, None]
    column_idx = jnp.arange(TOKENS)[None, :]
    hot_mask = column_idx < CAPACITY
    hot_local = (source_dev * CAPACITY + column_idx + owner_shift[hot_owner]) % ADAPTERS
    flat_index = start_offset + source_dev * spare_rows + column_idx - CAPACITY
    other_owner = (hot_owner + 1 + flat_index % (GROUP_SIZE - 1)) % GROUP_SIZE
    visit_count = flat_index // (GROUP_SIZE - 1)
    other_local = (visit_count + owner_shift[other_owner]) % ADAPTERS
    owner_ids = jnp.where(hot_mask, hot_owner, other_owner)
    local_ids = jnp.where(hot_mask, hot_local, other_local)
    id_table = owner_ids * ADAPTERS + local_ids
    perm_keys = jax.random.split(key_perm, GROUP_SIZE)
    perm_rows = jax.vmap(lambda perm_key: jax.random.permutation(perm_key, TOKENS))(perm_keys)
    id_table = jnp.take_along_axis(id_table, perm_rows, axis=1)
    return id_table.reshape(-1).astype(jnp.int32)


def normal_bf16(key_one, arr_shape, spread):
    return (jax.random.normal(key_one, arr_shape, jnp.float32) * spread).astype(jnp.bfloat16)


def setup_inputs(seed: int = 0, part: int = 0) -> dict:
    base_key = jax.random.key(seed)
    part_key = jax.random.fold_in(base_key, part)
    shared_keys = jax.random.split(base_key, 9)
    part_keys = jax.random.split(part_key, 3)
    b_std = 0.3 * LORA_RANK ** -0.5 / LORA_SCALE
    d_std = MODEL_DIM ** -0.5
    f_std = HIDDEN_DIM ** -0.5
    return {
        'x': normal_bf16(part_keys[0], (PART_TOKENS, MODEL_DIM), 1.0),
        'adapter_id': draw_ids(part_keys[1]),
        'dout': normal_bf16(part_keys[2], (PART_TOKENS, MODEL_DIM), 1.0),
        'w_gate': normal_bf16(shared_keys[0], (MODEL_DIM, HIDDEN_DIM), d_std),
        'w_up': normal_bf16(shared_keys[1], (MODEL_DIM, HIDDEN_DIM), d_std),
        'w_down': normal_bf16(shared_keys[2], (HIDDEN_DIM, MODEL_DIM), f_std),
        'a_gate': normal_bf16(shared_keys[3], (NUM_ADAPTERS, MODEL_DIM, LORA_RANK), d_std),
        'b_gate': normal_bf16(shared_keys[4], (NUM_ADAPTERS, LORA_RANK, HIDDEN_DIM), b_std),
        'a_up': normal_bf16(shared_keys[5], (NUM_ADAPTERS, MODEL_DIM, LORA_RANK), d_std),
        'b_up': normal_bf16(shared_keys[6], (NUM_ADAPTERS, LORA_RANK, HIDDEN_DIM), b_std),
        'a_down': normal_bf16(shared_keys[7], (NUM_ADAPTERS, HIDDEN_DIM, LORA_RANK), f_std),
        'b_down': normal_bf16(shared_keys[8], (NUM_ADAPTERS, LORA_RANK, MODEL_DIM), b_std),
    }


def bf16_cast(values):
    return values.astype(jnp.bfloat16).astype(jnp.float32)


def reference(x, adapter_id, dout, w_gate, w_up, w_down, a_gate, b_gate, a_up, b_up, a_down, b_down):
    gate_wt = w_gate.astype(jnp.float32)
    up_wt = w_up.astype(jnp.float32)
    down_wt = w_down.astype(jnp.float32)
    model_width = x.shape[1]
    num_blocks = x.shape[0] // BLOCK_ROWS

    def block_step(grad_sums, block_in):
        x_blk, id_blk, dy_blk = block_in
        x_rows = x_blk.astype(jnp.float32)
        dy_rows = dy_blk.astype(jnp.float32)
        ag_rows = a_gate[id_blk].astype(jnp.float32)
        bg_rows = b_gate[id_blk].astype(jnp.float32)
        au_rows = a_up[id_blk].astype(jnp.float32)
        bu_rows = b_up[id_blk].astype(jnp.float32)
        ad_rows = a_down[id_blk].astype(jnp.float32)
        bd_rows = b_down[id_blk].astype(jnp.float32)
        p_gate = bf16_cast(jnp.einsum('td,tdr->tr', x_rows, ag_rows))
        p_up = bf16_cast(jnp.einsum('td,tdr->tr', x_rows, au_rows))
        e_gate = bf16_cast(LORA_SCALE * jnp.einsum('tr,trf->tf', p_gate, bg_rows))
        e_up = bf16_cast(LORA_SCALE * jnp.einsum('tr,trf->tf', p_up, bu_rows))
        gate_pre = jnp.dot(x_rows, gate_wt) + e_gate
        up_pre = jnp.dot(x_rows, up_wt) + e_up
        gate_sig = jax.nn.sigmoid(gate_pre)
        gate_act = gate_pre * gate_sig
        hidden = bf16_cast(gate_act * up_pre)
        p_down = bf16_cast(jnp.einsum('tf,tfr->tr', hidden, ad_rows))
        e_down = bf16_cast(LORA_SCALE * jnp.einsum('tr,trd->td', p_down, bd_rows))
        out_blk = (x_rows + jnp.dot(hidden, down_wt) + e_down).astype(jnp.bfloat16)
        q_down = bf16_cast(LORA_SCALE * jnp.einsum('td,trd->tr', dy_rows, bd_rows))
        dh_lora = bf16_cast(jnp.einsum('tr,tfr->tf', q_down, ad_rows))
        d_hidden = jnp.einsum('td,fd->tf', dy_rows, down_wt) + dh_lora
        d_gate = bf16_cast(d_hidden * up_pre * gate_sig * (1.0 + gate_pre * (1.0 - gate_sig)))
        d_up = bf16_cast(d_hidden * gate_act)
        q_gate = bf16_cast(LORA_SCALE * jnp.einsum('tf,trf->tr', d_gate, bg_rows))
        q_up = bf16_cast(LORA_SCALE * jnp.einsum('tf,trf->tr', d_up, bu_rows))
        dx_lora = bf16_cast(jnp.einsum('tr,tdr->td', q_gate, ag_rows) + jnp.einsum('tr,tdr->td', q_up, au_rows))
        dx_blk = (dy_rows + jnp.einsum('tf,df->td', d_gate, gate_wt) + jnp.einsum('tf,df->td', d_up, up_wt) + dx_lora).astype(jnp.bfloat16)
        updates = (
            jnp.einsum('td,tr->tdr', x_rows, q_gate),
            LORA_SCALE * jnp.einsum('tr,tf->trf', p_gate, d_gate),
            jnp.einsum('td,tr->tdr', x_rows, q_up),
            LORA_SCALE * jnp.einsum('tr,tf->trf', p_up, d_up),
            jnp.einsum('tf,tr->tfr', hidden, q_down),
            LORA_SCALE * jnp.einsum('tr,td->trd', p_down, dy_rows),
        )
        new_sums = tuple(grad_acc.at[id_blk].add(grad_upd) for grad_acc, grad_upd in zip(grad_sums, updates))
        return new_sums, (out_blk, dx_blk)

    init_sums = tuple(jnp.zeros(weight.shape, jnp.float32) for weight in (a_gate, b_gate, a_up, b_up, a_down, b_down))
    blocks_in = (
        x.reshape(num_blocks, BLOCK_ROWS, model_width),
        adapter_id.reshape(num_blocks, BLOCK_ROWS),
        dout.reshape(num_blocks, BLOCK_ROWS, model_width),
    )
    grad_sums, (out_rows, dx_rows) = lax.scan(block_step, init_sums, blocks_in)
    return (out_rows.reshape(-1, model_width), dx_rows.reshape(-1, model_width), grad_sums[0], grad_sums[1], grad_sums[2], grad_sums[3], grad_sums[4], grad_sums[5])
```

```python
import functools

import jax
import jax.numpy as jnp
from jax import lax
from jax.experimental import pallas as pl
from jax.experimental.pallas import tpu as pltpu
from jax.sharding import PartitionSpec as P

ALPHA = 32
LANES = 128
F32 = jnp.float32
BF16 = jnp.bfloat16
VMEM_LIMIT = 62 * 1024 * 1024


def dot_nn(a, b):
    return lax.dot_general(a, b, (((1,), (0,)), ((), ())), preferred_element_type=F32)


def dot_nt(a, b):
    return lax.dot_general(a, b, (((1,), (1,)), ((), ())), preferred_element_type=F32)


def dot_tn(a, b):
    return lax.dot_general(a, b, (((0,), (0,)), ((), ())), preferred_element_type=F32)


def whole(shape):
    return pl.BlockSpec(shape, lambda *_: (0,) * len(shape), pipeline_mode=pl.Buffered(1))


def params(**kw):
    return pltpu.CompilerParams(vmem_limit_bytes=VMEM_LIMIT, **kw)


def cost(flops, nbytes):
    return pl.CostEstimate(flops=flops, bytes_accessed=nbytes, transcendentals=0)


MESH_ID = pl.DeviceIdType.MESH


class Exchange:
    def __init__(self, groups, items, collective_id):
        self.groups, self.items, self.collective_id = groups, items, collective_id
        self.arrays = [a for _, a, _ in items]
        self.rows = [a.shape[0] // {'block': groups, 'some': max(n, 1), 'all': 1}[kind] for kind, a, n in items]
        self.out_shape = [jax.ShapeDtypeStruct((groups * b, a.shape[1]), a.dtype) for b, a in zip(self.rows, self.arrays, strict=True)]
        self.specs = [pl.BlockSpec(memory_space=pl.ANY)] * len(items)
        self.scratch = [pltpu.SemaphoreType.DMA((len(items),))] * 2

    def params(self):
        return params(collective_id=self.collective_id, has_side_effects=True)

    def start(self, srcs, dsts, send, recv):
        groups = self.groups
        me = lax.axis_index('data')
        barrier = pltpu.get_barrier_semaphore()

        def signal(i, _):
            pl.semaphore_signal(barrier, inc=1, device_id={'data': lax.rem(me + i, groups)}, device_id_type=MESH_ID)
            return 0

        lax.fori_loop(1, groups, signal, 0)
        pl.semaphore_wait(barrier, groups - 1)
        for k, (kind, _, n) in enumerate(self.items):
            b = self.rows[k]

            def part(dest, k=k, b=b, kind=kind):
                return srcs[k] if kind == 'all' else srcs[k].at[pl.ds(dest * b, b)]

            def copy(dest, k=k, b=b, part=part):
                pltpu.make_async_remote_copy(
                    src_ref=part(dest), dst_ref=dsts[k].at[pl.ds(me * b, b)], send_sem=send.at[k], recv_sem=recv.at[k],
                    device_id={'data': dest}, device_id_type=MESH_ID).start()

            def mine(k=k, b=b, part=part):
                pltpu.make_async_copy(part(me), dsts[k].at[pl.ds(me * b, b)], recv.at[k]).start()

            def step(i, _, copy=copy, kind=kind, n=n):
                dest = lax.rem(me + i, groups)
                if kind == 'some' and n < groups:
                    pl.when(dest < n)(lambda: copy(dest))
                else:
                    copy(dest)
                return 0

            lax.fori_loop(1, groups, step, 0)
            if kind == 'some' and n < groups:
                pl.when(me < n)(mine)
            else:
                mine()

    def finish(self, srcs, dsts, send, recv):
        groups = self.groups
        me = lax.axis_index('data')
        for k, (kind, _, n) in enumerate(self.items):
            b = self.rows[k]

            def took(count, sem, k=k, b=b):
                ref = dsts[k].at[pl.ds(0, count * b)]
                pltpu.make_async_copy(ref, ref, sem.at[k]).wait()

            if kind == 'some' and n < groups:
                pl.when(me < n)(lambda took=took: took(groups, recv))
                pl.when(me < n)(lambda took=took, n=n: took(n - 1, send))
                pl.when(me >= n)(lambda took=took, n=n: took(n, send))
            else:
                took(groups, recv)
                took(groups - 1, send)


def exchange_kernel(*refs, xchg):
    n = len(xchg.items)
    srcs, dsts, sems = refs[:n], refs[n:2 * n], refs[2 * n:]
    xchg.start(srcs, dsts, *sems)
    xchg.finish(srcs, dsts, *sems)


def exchange_only(xchg):
    return pl.pallas_call(
        functools.partial(exchange_kernel, xchg=xchg),
        in_specs=xchg.specs,
        out_specs=xchg.specs,
        out_shape=xchg.out_shape,
        scratch_shapes=xchg.scratch,
        compiler_params=xchg.params(),
        cost_estimate=cost(10**10, 10**7),
        name='exchange',
    )(*xchg.arrays)


def route_kernel(own_ref, ids_ref, x_ref, d_ref, xp_ref, dp_ref, meta_ref, pt_ref, *, groups):
    tokens = ids_ref.shape[1]
    quota = tokens // groups
    sq = (tokens, tokens)
    row = lax.broadcasted_iota(jnp.int32, sq, 0)
    col = lax.broadcasted_iota(jnp.int32, sq, 1)
    slot_owner_r = lax.div(row, jnp.int32(quota))
    slot_owner_c = lax.div(col, jnp.int32(quota))
    own_c = jnp.broadcast_to(own_ref[...], sq)
    own_r = own_c.T
    one = jnp.float32(1)
    zero = jnp.float32(0)

    def count(cond, axis):
        return jnp.sum(jnp.where(cond, one, zero), axis=axis, keepdims=True)

    rank_c = count((own_c == own_r) & (row < col), 0)
    rank_r = count((own_c == own_r) & (col < row), 1)
    over_c = rank_c >= quota
    over_r = jnp.broadcast_to(rank_r, sq) >= quota
    over_idx_c = count(over_r & (row < col), 0)
    held_r = count(own_c == slot_owner_r, 1)
    held_c = count(own_r == slot_owner_c, 0)
    place_r = (row - slot_owner_r * quota).astype(F32)
    place_c = (col - slot_owner_c * quota).astype(F32)
    free_r = place_r >= held_r
    free_c = place_c >= held_c
    free_idx_r = count(free_c & (col < row), 1)
    own_cf = own_c.astype(F32)
    near = (own_cf * quota + rank_c) == row.astype(F32)
    spare = free_r & (free_idx_r == over_idx_c)
    over_cf = jnp.broadcast_to(jnp.where(over_c, one, zero), sq)
    perm = jnp.where(over_cf > 0, jnp.where(spare, one, zero), jnp.where(near, one, zero))
    perm_b = perm.astype(BF16)
    xp_ref[...] = dot_nn(perm_b, x_ref[...]).astype(BF16)
    dp_ref[...] = dot_nn(perm_b, d_ref[...]).astype(BF16)
    pt_ref[...] = perm.T.astype(BF16)
    ids_r = jnp.sum(perm * ids_ref[...].astype(F32), axis=1, keepdims=True)
    hot_max = jnp.max(jnp.where(over_cf > 0, own_cf, -one))
    hot_min = jnp.min(jnp.where(over_cf > 0, own_cf, one * groups))
    lane = lax.broadcasted_iota(jnp.int32, meta_ref.shape, 1)
    meta_ref[...] = jnp.where(lane == 0, ids_r, jnp.where(lane == 1, hot_max, hot_min))


def route(ids, owner, x, dy, groups):
    tokens, width = x.shape
    return pl.pallas_call(
        functools.partial(route_kernel, groups=groups),
        out_shape=(
            jax.ShapeDtypeStruct(x.shape, BF16),
            jax.ShapeDtypeStruct(dy.shape, BF16),
            jax.ShapeDtypeStruct((tokens, LANES), F32),
            jax.ShapeDtypeStruct((tokens, tokens), BF16),
        ),
        compiler_params=params(),
        cost_estimate=cost(4 * tokens * tokens * width, 8 * tokens * width),
        name='route',
    )(owner.reshape(1, tokens), ids.reshape(1, tokens), x, dy)


def back_kernel(pt_ref, out_in, dxa_in, dxb_in, out_ref, dx_ref):
    pt = pt_ref[...]
    half = dxa_in.shape[1]
    out_ref[...] = dot_nn(pt, out_in[...]).astype(BF16)
    dx_ref[:, :half] = dot_nn(pt, dxa_in[...]).astype(BF16)
    dx_ref[:, half:] = dot_nn(pt, dxb_in[...]).astype(BF16)


def back(pt, out, dxa, dxb):
    tokens, width = out.shape
    return pl.pallas_call(
        back_kernel,
        out_shape=[jax.ShapeDtypeStruct(out.shape, BF16)] * 2,
        compiler_params=params(),
        cost_estimate=cost(4 * tokens * tokens * width, 8 * tokens * width),
        name='back',
    )(pt, out, dxa, dxb)


def gu_kernel(x_ref, wg_ref, wu_ref, *refs, xchg, steps, old):
    n = len(xchg.items)
    srcs, refs = refs[:n], refs[n + old:]
    (g_ref, u_ref), dsts, sems = refs[:2], refs[2:n + 2], refs[n + 2:]
    step = pl.program_id(0)

    @pl.when(step == 0)
    def _():
        xchg.start(srcs, dsts, *sems)

    x = x_ref[...]
    g_ref[...] = dot_nn(x, wg_ref[...])
    u_ref[...] = dot_nn(x, wu_ref[...])

    @pl.when(step == steps - 1)
    def _():
        xchg.finish(srcs, dsts, *sems)


def gate_up(x, wg, wu, tile, start, steps, total, xchg, old=()):
    tokens, width = x.shape
    cols = tile * steps
    at = lambda i: (0, start + i)
    n = len(xchg.items)
    return pl.pallas_call(
        functools.partial(gu_kernel, xchg=xchg, steps=steps, old=len(old)),
        grid=(steps,),
        in_specs=[whole(x.shape)] + [pl.BlockSpec((width, tile), at)] * 2 + xchg.specs + [pl.BlockSpec(memory_space=pl.ANY)] * len(old),
        out_specs=[pl.BlockSpec((tokens, tile), at)] * 2 + xchg.specs,
        out_shape=[jax.ShapeDtypeStruct((tokens, tile * total), F32)] * 2 + xchg.out_shape,
        scratch_shapes=xchg.scratch,
        input_output_aliases={3 + n + k: k for k in range(len(old))},
        compiler_params=xchg.params(),
        cost_estimate=cost(4 * tokens * width * cols, 4 * width * cols + 8 * tokens * cols),
        name='gate_up',
    )(x, wg, wu, *xchg.arrays, *old)


def adapter_mask(scal_ref, meta_ref, rank, n_local, cols):
    me, hot = scal_ref[0], scal_ref[1]
    shape = (meta_ref.shape[0], cols)
    lid = jnp.broadcast_to(meta_ref[:, 0:1], shape).astype(jnp.int32)
    col = lax.broadcasted_iota(jnp.int32, shape, 1)
    block = lax.div(col, jnp.int32(rank))
    mine = me * n_local + block
    theirs = jnp.where(hot == me, -1, hot * n_local + block - n_local)
    return jnp.where(block < n_local, mine, theirs) == lid


def mid_kernel(*refs, names, cfg, xchg):
    r = dict(zip(names, refs, strict=True))
    first, last, steps = cfg['first'], cfg['last'], cfg['steps']
    rank, n_local, scale, groups = cfg['rank'], cfg['n_local'], cfg['scale'], cfg['groups']
    half = rank * n_local
    cap = cfg['cap']
    step = pl.program_id(0)
    count = len(xchg.items) if xchg else 0
    srcs = [r['x_src%d' % k] for k in range(count)]
    dsts = [r['x_dst%d' % k] for k in range(count)]

    def scaled(v):
        return v if scale == 1.0 else v * scale

    def both(name):
        return jnp.concatenate([r[name + '_own'][...], r[name + '_hot'][...]], axis=0)

    def packed(values, tail):
        parts = []
        for v in values:
            rows = dot_nn(r['sel'][...], v[:, half:])
            parts.append(sum(rows[:, k * rank:(k + 1) * rank] for k in range(n_local)))
        return jnp.concatenate([*parts, tail], axis=1).astype(BF16)

    @pl.when(step == 0)
    def _():
        if xchg:
            xchg.start(srcs, dsts, r['send'], r['recv'])
        if first:
            me, hot = r['scal'][0], r['scal'][1]
            mask = adapter_mask(r['scal'], r['meta'], rank, n_local, 2 * half)
            r['pg'][...] = jnp.where(mask, dot_nt(r['x'][...], both('ag')), 0.0).astype(BF16)
            r['pu'][...] = jnp.where(mask, dot_nt(r['x'][...], both('au')), 0.0).astype(BF16)
            r['qd'][...] = jnp.where(mask, scaled(dot_nt(r['dy'][...], both('bd'))), 0.0).astype(BF16)
            for name in ('pd_acc', 'qg_acc', 'qu_acc', 'out_acc'):
                r[name][...] = jnp.zeros_like(r[name])
            tokens = r['meta'].shape[0]
            sq = (tokens, tokens)
            low = (me * n_local).astype(F32)
            far = lambda lid: jnp.where((lid < low) | (lid >= low + n_local), 1.0, 0.0)
            lid_r = jnp.broadcast_to(r['meta'][:, 0:1], sq)
            before = lax.broadcasted_iota(jnp.int32, sq, 0) < lax.broadcasted_iota(jnp.int32, sq, 1)
            nth = jnp.sum(jnp.where(before, far(lid_r), 0.0), axis=0, keepdims=True)
            lid_c = lid_r.T[0:1]
            far_c = far(lid_c)
            slot = lax.broadcasted_iota(jnp.int32, (cap, tokens), 0).astype(F32)
            sel = jnp.where(slot == nth, jnp.broadcast_to(far_c, (cap, tokens)), 0.0)
            r['sel'][...] = sel.astype(BF16)
            which = jnp.sum(sel * (lid_c - (hot * n_local).astype(F32)), axis=1, keepdims=True)
            lane = lax.broadcasted_iota(jnp.int32, (cap, rank), 1)
            tail = jnp.where(lane == 0, which, jnp.where(lane == 1, jnp.sum(far_c), 0.0))
            r['prow'][...] = packed([r['pg'][...], r['pu'][...], r['qd'][...]], tail)
            for k, name in enumerate(('pg', 'pu', 'qd')):
                r['left'][k] = jnp.concatenate([r[name][:, :half].astype(F32).T, sel], axis=0).astype(BF16)
            part = r['x'].shape[1] // groups
            for k, name in enumerate(('x', 'dy')):
                rows = dot_nn(r['sel'][...], r[name][...]).astype(BF16)
                for d in range(groups):
                    r['drow'][d * cap:(d + 1) * cap, k * part:(k + 1) * part] = rows[:, d * part:(d + 1) * part]
        else:
            for name in ('pg', 'pu', 'qd', 'sel', 'left', 'pd_acc', 'qg_acc', 'qu_acc', 'out_acc'):
                r[name][...] = r[name + '_in'][...]

    pg, pu, qd = r['pg'][...], r['pu'][...], r['qd'][...]
    bg, bu, ad, wd = both('bg'), both('bu'), both('ad'), r['wd'][...]
    g = r['g'][...] + scaled(dot_nn(pg, bg)).astype(BF16).astype(F32)
    u = r['u'][...] + scaled(dot_nn(pu, bu)).astype(BF16).astype(F32)
    dh = dot_nt(r['dy'][...], wd) + dot_nn(qd, ad).astype(BF16).astype(F32)
    sig = jax.nn.sigmoid(g)
    act = g * sig
    h = (act * u).astype(BF16)
    dg = (dh * u * sig * (1.0 + g * (1.0 - sig))).astype(BF16)
    du = (dh * act).astype(BF16)
    r['dg'][...] = dg
    r['du'][...] = du
    r['pd_acc'][...] += dot_nt(h, ad)
    r['qg_acc'][...] += dot_nt(dg, bg)
    r['qu_acc'][...] += dot_nt(du, bu)
    r['out_acc'][...] += dot_nn(h, wd)
    piece = h.shape[1] // 2
    for k, (name, left, v) in enumerate((('gad', 2, h), ('gbg', 0, dg), ('gbu', 1, du))):
        both_rows = dot_nn(r['left'][left], v)
        r[name][...] = both_rows[:half] if name == 'gad' else scaled(both_rows[:half])
        for i in range(2):
            r['rows'][i * cap:(i + 1) * cap, k * piece:(k + 1) * piece] = both_rows[half:, i * piece:(i + 1) * piece].astype(BF16)

    @pl.when(step == steps - 1)
    def _():
        if last:
            mask = adapter_mask(r['scal'], r['meta'], rank, n_local, 2 * half)
            pd = jnp.where(mask, r['pd_acc'][...], 0.0).astype(BF16)
            qg = jnp.where(mask, scaled(r['qg_acc'][...]), 0.0).astype(BF16)
            qu = jnp.where(mask, scaled(r['qu_acc'][...]), 0.0).astype(BF16)
            r['qg'][...] = qg
            r['qu'][...] = qu
            e_down = scaled(dot_nn(pd, both('bd'))).astype(BF16).astype(F32)
            r['out'][...] = (r['x'][...].astype(F32) + r['out_acc'][...] + e_down).astype(BF16)
            r['gag'][...] = dot_tn(qg[:, :half], r['x'][...])
            r['gau'][...] = dot_tn(qu[:, :half], r['x'][...])
            r['gbd'][...] = scaled(dot_tn(pd[:, :half], r['dy'][...]))
            r['prow'][...] = packed([qg, qu, pd], jnp.zeros((cap, rank), F32))
        if xchg:
            xchg.finish(srcs, dsts, r['send'], r['recv'])


def mid(arrays, cfg, xchg=None):
    first, last = cfg['first'], cfg['last']
    tile, start, steps, cap, groups = cfg['tile'], cfg['start'], cfg['steps'], cfg['cap'], cfg['groups']
    tokens, width = arrays['x'].shape
    hidden = arrays['wd'].shape[0]
    rank = cfg['rank']
    half = rank * cfg['n_local']
    cols = tile * steps
    at = lambda i: (0, start + i)
    anywhere = pl.BlockSpec(memory_space=pl.ANY)
    ins, specs, aliases = [], [], {}

    def take(name, spec):
        ins.append(name)
        specs.append(spec)

    take('scal', pl.BlockSpec(memory_space=pltpu.SMEM))
    for name in ('meta', 'x', 'dy'):
        take(name, whole(arrays[name].shape))
    for name in ('ag', 'au', 'bd') if first else ('bd',):
        take(name + '_own', whole((half, width)))
        take(name + '_hot', whole((half, width)))
    carry = [('pg', BF16, (tokens, 2 * half)), ('pu', BF16, (tokens, 2 * half)), ('qd', BF16, (tokens, 2 * half)),
             ('sel', BF16, (cap, tokens)), ('left', BF16, (3, half + cap, tokens)),
             ('pd_acc', F32, (tokens, 2 * half)), ('qg_acc', F32, (tokens, 2 * half)), ('qu_acc', F32, (tokens, 2 * half)),
             ('out_acc', F32, (tokens, width))]
    if not first:
        for name, _, shape in carry:
            take(name + '_in', whole(shape))
    for name in ('bg', 'bu', 'ad'):
        take(name + '_own', pl.BlockSpec((half, tile), at))
        take(name + '_hot', pl.BlockSpec((half, tile), at))
    take('wd', pl.BlockSpec((tile, width), lambda i: (start + i, 0)))
    for name in ('g', 'u'):
        take(name, pl.BlockSpec((tokens, tile), at))
    outs, ospecs, oshapes = [], [], []

    def give(name, shape, dtype, spec):
        outs.append(name)
        ospecs.append(spec)
        oshapes.append(jax.ShapeDtypeStruct(shape, dtype))

    wide = [(name, (half, hidden), F32, half) for name in ('gbg', 'gbu', 'gad')] + [(name, (tokens, hidden), BF16, tokens) for name in ('dg', 'du')]
    for name, shape, dtype, n in wide:
        give(name, shape, dtype, pl.BlockSpec((n, tile), at))
        if not first:
            aliases[len(ins)] = outs.index(name)
            take(name + '_in', anywhere)
    give('rows', (2 * steps * cap, 3 * tile // 2), BF16, pl.BlockSpec((2 * cap, 3 * tile // 2), lambda i: (i, 0)))
    give('prow', (cap, 4 * rank), BF16, whole((cap, 4 * rank)))
    scratch = []
    if first:
        give('drow', (groups * cap, 2 * width // groups), BF16, whole((groups * cap, 2 * width // groups)))
    if last:
        give('out', (tokens, width), BF16, whole((tokens, width)))
        for name in ('qg', 'qu'):
            give(name, (tokens, 2 * half), BF16, whole((tokens, 2 * half)))
        for name in ('gag', 'gau', 'gbd'):
            give(name, (half, width), F32, whole((half, width)))
        scratch = [(name, pltpu.VMEM(shape, dtype)) for name, dtype, shape in carry]
    else:
        for name, dtype, shape in carry:
            give(name, shape, dtype, whole(shape))
    if xchg:
        for k, (array, shape) in enumerate(zip(xchg.arrays, xchg.out_shape, strict=True)):
            arrays = {**arrays, 'x_src%d' % k: array}
            take('x_src%d' % k, anywhere)
            give('x_dst%d' % k, shape.shape, shape.dtype, anywhere)
        scratch += list(zip(('send', 'recv'), xchg.scratch, strict=True))
    names = ins + outs + [name for name, _ in scratch]
    results = pl.pallas_call(
        functools.partial(mid_kernel, names=names, cfg=cfg, xchg=xchg),
        grid=(steps,),
        in_specs=specs,
        out_specs=ospecs,
        out_shape=oshapes,
        scratch_shapes=[s for _, s in scratch],
        input_output_aliases=aliases,
        compiler_params=xchg.params() if xchg else params(),
        cost_estimate=cost(4 * tokens * width * cols, 2 * width * cols),
        name='mid',
    )(*[arrays[name] for name in ins])
    return dict(zip(outs, results, strict=True))


def dx_kernel(dy_ref, qg_ref, qu_ref, ag_own, ag_hot, au_own, au_hot, dg_ref, du_ref, wg_ref, wu_ref, *refs, xchg, steps):
    n = len(xchg.items)
    srcs, dx_ref, dsts, send, recv = refs[:n], refs[n], refs[n + 1:2 * n + 1], refs[-2], refs[-1]
    step = pl.program_id(0)

    @pl.when(step == 0)
    def _():
        xchg.start(srcs, dsts, send, recv)

    ag = jnp.concatenate([ag_own[...], ag_hot[...]], axis=0)
    au = jnp.concatenate([au_own[...], au_hot[...]], axis=0)
    low = (dot_nn(qg_ref[...], ag) + dot_nn(qu_ref[...], au)).astype(BF16).astype(F32)
    base = dot_nt(dg_ref[...], wg_ref[...]) + dot_nt(du_ref[...], wu_ref[...])
    dx_ref[...] = (dy_ref[...].astype(F32) + base + low).astype(BF16)

    @pl.when(step == steps - 1)
    def _():
        xchg.finish(srcs, dsts, send, recv)


def dx_part(dy, qg, qu, ag_own, ag_hot, au_own, au_hot, dg, du, wg, wu, tile, start, steps, xchg):
    tokens = dy.shape[0]
    hidden = dg.shape[1]
    half = ag_own.shape[0]
    width = steps * tile
    at = lambda i: (0, start + i)
    return pl.pallas_call(
        functools.partial(dx_kernel, xchg=xchg, steps=steps),
        grid=(steps,),
        in_specs=[pl.BlockSpec((tokens, tile), at), whole(qg.shape), whole(qu.shape)]
        + [pl.BlockSpec((half, tile), at)] * 4
        + [whole(dg.shape), whole(du.shape)]
        + [pl.BlockSpec((tile, hidden), lambda i: (start + i, 0))] * 2
        + xchg.specs,
        out_specs=[pl.BlockSpec((tokens, tile), lambda i: (0, i))] + xchg.specs,
        out_shape=[jax.ShapeDtypeStruct((tokens, width), BF16)] + xchg.out_shape,
        scratch_shapes=xchg.scratch,
        compiler_params=xchg.params(),
        cost_estimate=cost(4 * tokens * width * hidden, 4 * width * hidden),
        name='dx',
    )(dy, qg, qu, ag_own, ag_hot, au_own, au_hot, dg, du, wg, wu, *xchg.arrays)


def slice_kernel(scal_ref, rows_ref, early_ref, *refs, rank, n_local, count, scale, deep):
    out_ref = refs[-1]
    half = rank * n_local
    piece = rows_ref.shape[1] // 3
    live = scal_ref[0] < count
    which = early_ref[:, 3 * rank:3 * rank + 1].astype(F32)

    def p(ref, k):
        v = ref[:, k * rank:(k + 1) * rank].astype(F32)
        return jnp.concatenate([jnp.where(which == i, v, 0.0) for i in range(n_local)], axis=1).astype(BF16)

    row = lambda k: rows_ref[:, k * piece:(k + 1) * piece]
    wide = (scale * dot_tn(p(early_ref, 0), row(1)), scale * dot_tn(p(early_ref, 1), row(2)), dot_tn(p(early_ref, 2), row(0)))
    for k, v in enumerate(wide):
        out_ref[k * half:(k + 1) * half, :piece] = jnp.where(live, v, 0.0)
    if deep:
        late_ref, drow_ref = refs[:2]
        x, dy = drow_ref[:, :deep], drow_ref[:, deep:]
        for k, v in enumerate((dot_tn(p(late_ref, 0), x), dot_tn(p(late_ref, 1), x), scale * dot_tn(p(late_ref, 2), dy))):
            out_ref[k * half:(k + 1) * half, piece:] = v


def slices(scal, rows, early, more, rank, n_local, count, scale):
    piece = rows.shape[1] // 3
    deep = more[1].shape[1] // 2 if more else 0
    return pl.pallas_call(
        functools.partial(slice_kernel, rank=rank, n_local=n_local, count=count, scale=scale, deep=deep),
        in_specs=[pl.BlockSpec(memory_space=pltpu.SMEM)] + [pl.BlockSpec(memory_space=pltpu.VMEM)] * (2 + len(more)),
        out_shape=jax.ShapeDtypeStruct((3 * rank * n_local, piece + deep), F32),
        compiler_params=params(),
        cost_estimate=cost(10**9, 10**7),
        name='slices',
    )(scal, rows, early, *more)


def add_kernel(flag_ref, *refs, half, heads):
    own, (more_a, more_b, more_d), outs = refs[:6], refs[6:9], refs[9:]
    step = pl.program_id(0)

    def put(k, out, mine, source):
        n, _, piece = source.shape
        for p in range(n):
            cols = slice(p * piece, (p + 1) * piece)
            out[:, cols] = mine[:, cols] + source[p, k * half:(k + 1) * half]

    for k in range(3):
        for mine, out, source, when in (
            (own[k], outs[k], more_a, step < heads), (own[k], outs[k], more_b, step >= heads), (own[3 + k], outs[3 + k], more_d, None)):
            hot = flag_ref[0] > 0
            pl.when(hot if when is None else hot & when)(functools.partial(put, k, out, mine, source))

        @pl.when(flag_ref[0] <= 0)
        def _(k=k):
            outs[k][...] = own[k][...]
            outs[3 + k][...] = own[3 + k][...]


def add_if(flag, own, more_a, more_b, half, piece, deep, n_a, n_b, groups):
    many, many_d = 1024 // piece, max(1, min(groups, 1024 // deep))
    tile, tile_d = many * piece, many_d * deep
    steps_a, steps_b, steps_d = n_a // many, n_b // many, groups // many_d
    wide = pl.BlockSpec((half, tile), lambda i, f: (0, i))
    narrow = pl.BlockSpec((half, tile_d), lambda i, f: (0, jnp.minimum(i, steps_d - 1)))
    cube = lambda a: a.reshape(groups, 3 * half, a.shape[1])
    rows = 3 * half
    specs = [wide] * 3 + [narrow] * 3
    return pl.pallas_call(
        functools.partial(add_kernel, half=half, heads=steps_a),
        grid_spec=pltpu.PrefetchScalarGridSpec(
            num_scalar_prefetch=1, grid=(steps_a + steps_b,),
            in_specs=specs + [
                pl.BlockSpec((many, rows, piece), lambda i, f: (jnp.minimum(i, steps_a - 1) * f[0], 0, 0)),
                pl.BlockSpec((many, rows, piece), lambda i, f: (jnp.maximum(i - steps_a, 0) * f[0], 0, 0)),
                pl.BlockSpec((many_d, rows, deep), lambda i, f: (jnp.minimum(i, steps_d - 1) * f[0], 0, piece // deep)),
            ],
            out_specs=specs),
        out_shape=[jax.ShapeDtypeStruct(a.shape, F32) for a in own],
        compiler_params=params(),
        name='add_if',
    )(flag, *own, cube(more_a), cube(more_b), cube(more_b))


def small_dot_kernel(a_ref, b_ref, o_ref, *, dot):
    @pl.when(pl.program_id(1) == 0)
    def _():
        o_ref[...] = jnp.zeros_like(o_ref)

    o_ref[...] += dot(a_ref[...], b_ref[...])


def small_dot(a, b, dot):
    a_at, b_at = (0 if dot is dot_tn else 1), (1 if dot is dot_nt else 0)
    depth, rows, cols = a.shape[a_at], a.shape[1 - a_at], b.shape[1 - b_at]
    bk, bn = min(depth, 512), min(cols, 512)
    a_spec = pl.BlockSpec((bk, rows), lambda j, k: (k, 0)) if a_at == 0 else pl.BlockSpec((rows, bk), lambda j, k: (0, k))
    b_spec = pl.BlockSpec((bk, bn), lambda j, k: (k, j)) if b_at == 0 else pl.BlockSpec((bn, bk), lambda j, k: (j, k))
    return pl.pallas_call(
        functools.partial(small_dot_kernel, dot=dot),
        grid=(cols // bn, depth // bk),
        in_specs=[a_spec, b_spec],
        out_specs=pl.BlockSpec((rows, bn), lambda j, k: (0, j)),
        out_shape=jax.ShapeDtypeStruct((rows, cols), F32),
        compiler_params=params(),
        name='small_dot',
    )(a, b)


def ring_path(x, ids, dy, wg, wu, wd, ag, bg, au, bu, ad, bd, groups, n_local, scale):
    rank = ag.shape[0] // n_local
    dot_nn_, dot_nt_, dot_tn_ = (functools.partial(small_dot, dot=d) for d in (dot_nn, dot_nt, dot_tn))
    half = rank * n_local
    me = lax.axis_index('data')
    ring = [(i, (i + 1) % groups) for i in range(groups)]
    shift = functools.partial(lax.ppermute, axis_name='data', perm=ring)
    tokens, width = x.shape
    hidden = wd.shape[0]

    def mask_of(k):
        owner = lax.rem(me - k + groups, groups)
        return ids[:, None] == owner * n_local + (jnp.arange(half) // rank)[None, :]

    def low(v, mask):
        return jnp.where(mask, v, 0.0).astype(BF16)

    def forward(k, carry):
        (cag, cbg, cau, cbu, cad, cbd), eg, eu, dh = carry
        mask = mask_of(k)
        eg = eg + scale * dot_nn_(low(dot_nt_(x, cag), mask), cbg)
        eu = eu + scale * dot_nn_(low(dot_nt_(x, cau), mask), cbu)
        dh = dh + dot_nn_(low(scale * dot_nt_(dy, cbd), mask), cad)
        return jax.tree.map(shift, (cag, cbg, cau, cbu, cad, cbd)), eg, eu, dh

    zero = jnp.zeros((tokens, hidden), F32)
    held, eg, eu, dh_low = lax.fori_loop(0, groups, forward, ((ag, bg, au, bu, ad, bd), zero, zero, zero))
    rounded = lambda v: v.astype(BF16).astype(F32)
    g = dot_nn_(x, wg) + rounded(eg)
    u = dot_nn_(x, wu) + rounded(eu)
    sig = jax.nn.sigmoid(g)
    act = g * sig
    h = (act * u).astype(BF16)
    dh = dot_nt_(dy, wd) + rounded(dh_low)
    dg = (dh * u * sig * (1.0 + g * (1.0 - sig))).astype(BF16)
    du = (dh * act).astype(BF16)

    def backward(k, carry):
        held, sums, e_down, dx_low = jax.tree.map(shift, carry[:2]) + carry[2:]
        cag, cbg, cau, cbu, cad, cbd = held
        mask = mask_of(k)
        pg, pu, pd = (low(dot_nt_(a, b), mask) for a, b in ((x, cag), (x, cau), (h, cad)))
        qg, qu, qd = (low(scale * dot_nt_(a, b), mask) for a, b in ((dg, cbg), (du, cbu), (dy, cbd)))
        e_down = e_down + scale * dot_nn_(pd, cbd)
        dx_low = dx_low + dot_nn_(qg, cag) + dot_nn_(qu, cau)
        more = (dot_tn_(qg, x), scale * dot_tn_(pg, dg), dot_tn_(qu, x), scale * dot_tn_(pu, du), dot_tn_(qd, h), scale * dot_tn_(pd, dy))
        return held, tuple(s + m for s, m in zip(sums, more, strict=True)), e_down, dx_low

    sums = tuple(jnp.zeros(a.shape, F32) for a in (ag, bg, au, bu, ad, bd))
    zero = jnp.zeros((tokens, width), F32)
    _, sums, e_down, dx_low = lax.fori_loop(1, groups + 1, backward, (held, sums, zero, zero))
    out = (x.astype(F32) + dot_nn_(h, wd) + rounded(e_down)).astype(BF16)
    dx = (dy.astype(F32) + dot_nt_(dg, wg) + dot_nt_(du, wu) + rounded(dx_low)).astype(BF16)
    return (out, dx, *sums)


def solution(mesh, force_ring=False, split=4 / 7):
    groups = mesh.shape['data']
    tok_spec = P(('rep', 'data'), None)
    own_spec = P('data', None, None)
    grad_spec = P(('rep', 'data'), None, None)

    def device_fn(x, ids, dy, wg, wu, wd, a_gate, b_gate, a_up, b_up, a_down, b_down):
        tokens, width = x.shape
        hidden = wg.shape[1]
        n_local, _, rank = a_gate.shape
        half = n_local * rank
        scale = ALPHA / rank
        me = lax.axis_index('data')
        tall = lambda a: jnp.transpose(a, (0, 2, 1)).reshape(half, a.shape[1])
        flat = lambda a: a.reshape(half, a.shape[2])
        own = dict(ag=tall(a_gate), bg=flat(b_gate), au=tall(a_up), bu=flat(b_up), ad=tall(a_down), bd=flat(b_down))

        xp, dp, meta, pt = route(ids, lax.div(ids, n_local), x, dy, groups)
        me_f = me.astype(F32)
        i_am_hot = (meta[0, 1] == me_f) & (meta[0, 2] == me_f)
        tile = 512
        tiles = hidden // tile
        head = max(2, min(tiles - 2, groups // 2, 2 * round(tiles * split / 2)))
        hot = lax.psum({k: jnp.where(i_am_hot, v, jnp.zeros_like(v)) for k, v in own.items()}, 'data')
        xr, meta_r = exchange_only(Exchange(groups, [('block', xp, 0), ('block', meta, 0)], 0))

        hot_all, low_all = meta_r[:, 1], meta_r[:, 2]
        hot_f = jnp.max(hot_all)
        hot_id = hot_f.astype(jnp.int32)
        scal = jnp.stack([me, hot_id]).astype(jnp.int32)
        flag = jnp.where(hot_id == me, 1, 0).astype(jnp.int32).reshape(1)

        cap = 24
        wider = 2 * tile if tiles % 2 == 0 else tile
        g, u, dr = gate_up(xr, wg, wu, wider, 0, hidden // wider, hidden // wider, Exchange(groups, [('block', dp, 0)], 1))
        arrays = dict(scal=scal, meta=meta_r, x=xr, dy=dr, wd=wd, g=g, u=u)
        for k in own:
            arrays[k + '_own'], arrays[k + '_hot'] = own[k], hot[k]
        cfg = dict(tile=tile, rank=rank, n_local=n_local, scale=scale, groups=groups, cap=cap)
        res_a = mid(arrays, dict(cfg, first=True, last=False, start=0, steps=head))
        n_a, n_b = 2 * head, 2 * (tiles - head)
        for k in ('pg', 'pu', 'qd', 'sel', 'left', 'pd_acc', 'qg_acc', 'qu_acc', 'out_acc', 'gbg', 'gbu', 'gad', 'dg', 'du'):
            arrays[k + '_in'] = res_a[k]
        res_b = mid(arrays, dict(cfg, first=False, last=True, start=head, steps=tiles - head), Exchange(
            groups, [('some', res_a['rows'], n_a), ('all', res_a['prow'], 0), ('block', res_a['drow'], 0)], 2))
        rows_a, early, drow = res_b['x_dst0'], res_b['x_dst1'], res_b['x_dst2']
        gather = lambda v: lax.all_gather(v, 'data', axis=0, tiled=True)
        more_a = gather(slices(scal, rows_a, early, [], rank, n_local, n_a, scale))
        dt = 256
        nd = width // dt // 2
        dx_args = (dr, res_b['qg'], res_b['qu'], own['ag'], hot['ag'], own['au'], hot['au'], res_b['dg'], res_b['du'], wg, wu, dt)
        dxa, rows_b, late = dx_part(*dx_args, 0, nd, Exchange(groups, [('some', res_b['rows'], n_b), ('all', res_b['prow'], 0)], 3))
        more_b = gather(slices(scal, rows_b, early, [late, drow], rank, n_local, n_b, scale))
        dxb, dxa_r, out_r = dx_part(*dx_args, nd, nd, Exchange(groups, [('block', dxa, 0), ('block', res_b['out'], 0)], 4))
        dxb_r, = exchange_only(Exchange(groups, [('block', dxb, 0)], 5))
        out, dx = back(pt, out_r, dxa_r, dxb_r)
        sums = [res_b[k] for k in ('gbg', 'gbu', 'gad', 'gag', 'gau', 'gbd')]
        gbg, gbu, gad, gag, gau, gbd = add_if(
            flag, sums, more_a, more_b, half, tile // 2, width // groups, n_a, n_b, groups)

        far = early[:, 3 * rank + 1]
        agree = jnp.all(((hot_all == hot_f) & (low_all == hot_f)) | (hot_all < 0))
        source = lax.div(jnp.arange(tokens), tokens // groups).astype(F32)
        knows = (hot_f < 0) | jnp.any((source == hot_f) & (hot_all == hot_f))
        ok = agree & knows & jnp.all(far.astype(F32) <= cap)
        fast = (out, dx, gag, gbg, gau, gbu, gad, gbd)

        back_tall = lambda a: jnp.transpose(a.reshape(n_local, rank, a.shape[1]), (0, 2, 1))
        back_flat = lambda a: a.reshape(n_local, rank, a.shape[1])

        def final(out, dx, gag, gbg, gau, gbu, gad, gbd):
            return out, dx, back_tall(gag), back_flat(gbg), back_tall(gau), back_flat(gbu), back_tall(gad), back_flat(gbd)

        def again(carry):
            names = ('ag', 'bg', 'au', 'bu', 'ad', 'bd')
            return (jnp.bool_(False), *final(*ring_path(x, ids, dy, wg, wu, wd, *(own[k] for k in names), groups, n_local, scale)))

        redo = jnp.bool_(True) if force_ring else jnp.logical_not(ok)
        return lax.while_loop(lambda c: c[0], again, (redo, *final(*fast)))[1:]

    return jax.shard_map(
        device_fn,
        mesh=mesh,
        in_specs=(tok_spec, P(('rep', 'data')), tok_spec) + (P(None, None),) * 3 + (own_spec,) * 6,
        out_specs=(tok_spec, tok_spec) + (grad_spec,) * 6,
        check_vma=False,
    )
```
